32 devices in a mesh: grp: 2 (over x), tp: 4 (over y, core), pp: 4 (over z).
Axes of the slice: x: 2, y: 2, z: 4, core: 2. Of those that a mesh axis runs over, the one named last changes fastest.
Arguments:
- tokens: bfloat16 [1024, 8192], P('grp', 'tp'), parts along dimension 0, may hold values from -12 to 12
- gain: bfloat16 [4, 8192], P('pp', 'tp'), may hold values from 0.099609375 to 1.8984375
- q_weight: bfloat16 [4, 8192, 4096], P('pp', None, 'tp'), may hold values from -0.5 to 0.5
- kv_weight: bfloat16 [4, 8192, 2048], P('pp', None, 'tp'), may hold values from -0.5 to 0.5
- out_weight: bfloat16 [4, 4096, 8192], P('pp', None, 'tp'), may hold values from -0.09375 to 0.09375
- page_table: int32 [4, 8, 128], P('pp'), may hold values from 0 to 1023, as said below
- segment_ids: int32 [1024], P('grp'), parts along dimension 0, may hold values from 0 to 2, never falling along the last dimension, each value on 1 to 256 neighbouring positions
Outputs:
- hidden: bfloat16 [1024, 8192], P(('grp', 'pp'), 'tp'), parts along dimension 0
- kv_cache: bfloat16 [4, 2048, 4, 256], P('pp', ('grp', 'tp')), parts along dimension 1
The draws below stay inside these ranges and needn't reach their ends.
There are 2 independent parts, one for each index of `grp`. The reference program is written for one: setup_inputs(seed, part) draws one part's arguments, and reference() takes and returns one part's arrays. A program takes and returns all parts, laid end to end along the dimension named above; an argument that names none is the same for every part. Nothing has to cross between parts.
Inputs may be any that keep to these rules, and one draw needn't show every extreme that they name: `page_table`: every entry of a layer's table is distinct and every one of the 1024 values occurs once. For each layer, head and micro-batch the 16 blocks form a run; in each run half of the devices receive exactly 8 pages and the others none, so each device receives exactly 256 pages of a layer.
All inputs are finite; a program needn't handle non-finite values.
Results may differ from the reference program's by a relative error of at most 0.017.
Values may be sent and summed in bfloat16 or wider, within the bound.
A program may use at most 128 MiB of HBM per device.

```python
import math
import jax
import jax.numpy as jnp
import numpy as np
from jax import lax

MODEL_WIDTH = 8192
QUERY_HEADS = 32
HEAD_SIZE = 128
KEY_VALUE_HEADS = 8
MICRO_BATCHES = 8
PAGE_TOKENS = 4
LAYER_COUNT = 4
PREFIX_TOKENS = 512
MB_BLOCKS = 16
PREFIX_BLOCKS = 128
MOST = 8
CACHE_PAGES = 256
N_TP = 4


def draw_tokens(key, part):
    first_key = jax.random.fold_in(key, 21)
    ramp_cols = 0.6 + 1.2 * jnp.arange(MODEL_WIDTH, dtype=jnp.float32) / MODEL_WIDTH
    rough = jax.random.normal(first_key, (PREFIX_TOKENS, MODEL_WIDTH), jnp.float32)
    return jnp.clip(rough * ramp_cols, -12.0, 12.0).astype(jnp.bfloat16)


def joint_weights(key):
    query_key = jax.random.fold_in(key, 11)
    key_value_random = jax.random.fold_in(key, 12)
    inverse_sqrt_width = math.sqrt(MODEL_WIDTH)
    key_value_rows = jax.random.normal(key_value_random, (LAYER_COUNT, MODEL_WIDTH, 2 * KEY_VALUE_HEADS * HEAD_SIZE), jnp.float32) / inverse_sqrt_width
    local_portion = jax.random.normal(query_key, (LAYER_COUNT, MODEL_WIDTH, QUERY_HEADS * HEAD_SIZE), jnp.float32) / inverse_sqrt_width
    query_matrix = local_portion
    return (jnp.clip(query_matrix, -0.5, 0.5), jnp.clip(key_value_rows, -0.5, 0.5))


def draw_q_weight(key, part):
    return joint_weights(key)[0].astype(jnp.bfloat16)


def draw_kv_weight(key, part):
    return joint_weights(key)[1].astype(jnp.bfloat16)


def draw_page_table(key, part):
    device_total = 2 * MB_BLOCKS // MOST
    half_count = device_total // 2
    running_total = KEY_VALUE_HEADS * MICRO_BATCHES
    pick_key = jax.random.fold_in(key, 31)
    shuffle_key = jax.random.fold_in(key, 32)
    slot_key = jax.random.fold_in(key, 33)
    device_scores = jax.random.randint(pick_key, (LAYER_COUNT, running_total // 2, device_total), 0, 1 << 20) * device_total + jnp.arange(device_total, dtype=jnp.int32)
    device_order = jnp.argsort(device_scores, axis=-1).astype(jnp.int32)
    chosen = jnp.stack([device_order[:, :, :half_count], device_order[:, :, half_count:]], axis=2)
    chosen = chosen.reshape(LAYER_COUNT, running_total, half_count)
    page_store = jnp.tile(chosen, (1, 1, MOST))
    mix_scores = jax.random.randint(shuffle_key, (LAYER_COUNT, running_total, MB_BLOCKS), 0, 1 << 20) * MB_BLOCKS + jnp.arange(MB_BLOCKS, dtype=jnp.int32)
    mixing_permutation = jnp.argsort(mix_scores, axis=-1).astype(jnp.int32)
    target_pages = jnp.take_along_axis(page_store, mixing_permutation, axis=-1).reshape(LAYER_COUNT, KEY_VALUE_HEADS * PREFIX_BLOCKS)
    onehot = (target_pages[:, :, None] == jnp.arange(device_total, dtype=jnp.int32)[None, None, :]).astype(jnp.int32)
    earlier = jnp.cumsum(onehot, axis=1) - onehot
    arrival = jnp.sum(earlier * onehot, axis=2)
    slot_scores = jax.random.randint(slot_key, (LAYER_COUNT, device_total, CACHE_PAGES), 0, 1 << 20) * CACHE_PAGES + jnp.arange(CACHE_PAGES, dtype=jnp.int32)
    slot_order = jnp.argsort(slot_scores, axis=-1).astype(jnp.int32).reshape(LAYER_COUNT, device_total * CACHE_PAGES)
    cache_page_index = jnp.take_along_axis(slot_order, target_pages * CACHE_PAGES + arrival, axis=1)
    return (target_pages * CACHE_PAGES + cache_page_index).reshape(LAYER_COUNT, KEY_VALUE_HEADS, PREFIX_BLOCKS).astype(jnp.int32)


def block_scale(rng, dims, shards, least, largest):
    def one(dim, parts):
        heights = jax.random.uniform(jax.random.fold_in(jax.random.fold_in(rng, 6), dim), (parts,), jnp.float32, least / len(shards), largest / len(shards))
        return jnp.repeat(jnp.exp(heights), dims[dim] // parts).reshape((-1,) + (1,) * (len(dims) - dim - 1))

    loudness = one(*shards[0])
    for cut in shards[1:]:
        loudness = loudness * one(*cut)
    return loudness


def profile(count, total, most, slope):
    portions = [(1 << 20) // math.isqrt(grade ** slope) + 1 for grade in range(2, count + 1)]
    rest, given = total - most - (count - 1), [1] * (count - 1)
    while rest > 0:
        free = [i for i in range(count - 1) if given[i] < most]
        mass, budget = sum([portions[i] for i in free]), rest
        for i in free:
            more = min(most - given[i], max(1, budget * portions[i] // mass), rest)
            given[i] = given[i] + more
            rest = rest - more
    return np.array([most] + given)


def ragged_sizes(rng, count, total, most, slope):
    if count == 2:
        one = jax.random.randint(rng, (), max(1, total - most), min(most, total - 1) + 1)
        return jnp.stack([one, total - one])
    tallies = jnp.asarray(profile(count, total, most, slope), jnp.int32)
    couples = (count - 1) // 2
    giver, taker = tallies[1:1 + 2 * couples:2], tallies[2:2 + 2 * couples:2]
    room = jnp.minimum(giver - 1, most - taker)
    moved = jax.random.randint(jax.random.fold_in(rng, 1), (couples,), 0, 1 << 20) % (room + 1)
    tallies = tallies.at[1:1 + 2 * couples:2].set(giver - moved).at[2:2 + 2 * couples:2].set(taker + moved)
    return tallies[jax.random.permutation(jax.random.fold_in(rng, 2), count)]


def normal_values(rng, shape, width, most, shards=(), held_as=jnp.bfloat16):
    values = jax.random.normal(rng, shape, jnp.float32) * width
    if len(shards) > 0:
        values = block_scale(rng, shape, shards, -0.22, 0.18) * values
    return jnp.clip(values, min=-most, max=most).astype(held_as)


def setup_inputs(seed: int = 0, part: int = 0) -> dict:
    splits = jax.random.split(jax.random.key(seed), 8)
    part_splits = jax.random.split(jax.random.fold_in(splits[7], part), 8)
    tokens = draw_tokens(jax.random.fold_in(jax.random.fold_in(splits[7], part), 71), part)
    gain = jnp.clip(1.0 + 0.18 * jax.random.normal(splits[1], (LAYER_COUNT, MODEL_WIDTH), jnp.float32), 0.099609375, 1.8984375).astype(jnp.bfloat16)
    q_weight = draw_q_weight(jax.random.fold_in(splits[7], 71), part)
    kv_weight = draw_kv_weight(jax.random.fold_in(splits[7], 71), part)
    out_weight = normal_values(splits[4], (LAYER_COUNT, QUERY_HEADS * HEAD_SIZE, MODEL_WIDTH), (QUERY_HEADS * HEAD_SIZE) ** -0.5, 0.09375, ((0, 4), (2, 4)))
    page_table = draw_page_table(jax.random.fold_in(splits[7], 71), part)
    segment_ids = jnp.searchsorted(jnp.cumsum(ragged_sizes(part_splits[6], 3, PREFIX_TOKENS, PREFIX_TOKENS // 2, 2)), jnp.arange(PREFIX_TOKENS), side="right").astype(jnp.int32)
    return {"tokens": tokens, "gain": gain, "q_weight": q_weight, "kv_weight": kv_weight, "out_weight": out_weight, "page_table": page_table, "segment_ids": segment_ids}


eps_norm = 1e-05

def reference(tokens, gain, q_weight, kv_weight, out_weight, page_table, segment_ids):
    query_group_width = QUERY_HEADS // KEY_VALUE_HEADS
    score_scale = 1.0 / math.sqrt(HEAD_SIZE)
    positions = jnp.arange(PREFIX_TOKENS, dtype=jnp.int32)
    allowed = (positions[None, :] <= positions[:, None]) & (segment_ids[None, :] == segment_ids[:, None])
    stream = tokens
    caches = []
    for layer_idx in range(LAYER_COUNT):
        widened = stream.astype(jnp.float32)
        mean_sq = lax.optimization_barrier(jnp.sum(widened * widened, axis=1, keepdims=True)) / MODEL_WIDTH
        normed = (widened * lax.rsqrt(mean_sq + eps_norm) * gain[layer_idx].astype(jnp.float32)).astype(jnp.bfloat16)
        query_matrix = jnp.dot(normed, q_weight[layer_idx], preferred_element_type=jnp.float32).astype(jnp.bfloat16)
        key_value_rows = jnp.dot(normed, kv_weight[layer_idx], preferred_element_type=jnp.float32).astype(jnp.bfloat16)
        key_value_heads = key_value_rows.reshape(PREFIX_TOKENS, KEY_VALUE_HEADS, 2, HEAD_SIZE).astype(jnp.float32)
        grouped_queries = query_matrix.reshape(PREFIX_TOKENS, KEY_VALUE_HEADS, query_group_width, HEAD_SIZE).astype(jnp.float32)
        scores = jnp.einsum('qgpd,kgd->gpqk', grouped_queries, key_value_heads[:, :, 0]) * score_scale
        scores = jnp.where(allowed[None, None], scores, -1e+30)
        row_max = lax.optimization_barrier(jnp.max(scores, axis=-1, keepdims=True))
        raised = jnp.exp(scores - row_max)
        weights = (raised / lax.optimization_barrier(jnp.sum(raised, axis=-1, keepdims=True))).astype(jnp.bfloat16)
        mixed_heads = jnp.einsum('gpqk,kgd->qgpd', weights.astype(jnp.float32), key_value_heads[:, :, 1])
        mixed_heads = mixed_heads.astype(jnp.bfloat16).reshape(PREFIX_TOKENS, QUERY_HEADS * HEAD_SIZE)
        update = jnp.dot(mixed_heads, out_weight[layer_idx], preferred_element_type=jnp.float32)
        stream = (widened + update).astype(jnp.bfloat16)
        page_contents = key_value_rows.reshape(PREFIX_BLOCKS, PAGE_TOKENS, KEY_VALUE_HEADS, 2 * HEAD_SIZE).transpose(2, 0, 1, 3).reshape(KEY_VALUE_HEADS * PREFIX_BLOCKS, PAGE_TOKENS, 2 * HEAD_SIZE)
        filled = jnp.zeros((N_TP * CACHE_PAGES, PAGE_TOKENS, 2 * HEAD_SIZE), jnp.bfloat16).at[page_table[layer_idx].reshape(-1)].set(page_contents)
        caches.append(filled)
    return (stream, jnp.stack(caches))
```

```python
import math

import jax
import jax.numpy as jnp
from jax import lax
from jax.sharding import PartitionSpec as P

MODEL_WIDTH = 8192
HEAD_SIZE = 128
KEY_VALUE_HEADS = 8
MICRO_BATCHES = 4
PAGE_TOKENS = 4


eps_norm = 1e-05


def partner_2(x, axis, apart):
    return lax.ppermute(x, axis, [(i, i ^ 1 << apart) for i in range(lax.axis_size(axis))])


def shifted(x, axis, by):
    peers = lax.axis_size(axis)
    pairs = [(i, i + by) for i in range(peers) if 0 <= i + by < peers]
    return lax.ppermute(x, axis, pairs)


def from_root(x, axis, root):
    mine = lax.axis_index(axis) == root
    return lax.psum(jnp.where(mine, x, jnp.zeros_like(x)), axis)


def own_pages(kv_buffer, page_rows, tp_rank, tensor_parallel_width, cache_page_count):
    row_total = kv_buffer.shape[0]
    blocks = row_total // PAGE_TOKENS
    copies = max(1, tensor_parallel_width // KEY_VALUE_HEADS)
    gathered = lax.all_gather(kv_buffer, "tp", axis=0, tiled=False)[::copies]
    head_width = 2 * HEAD_SIZE
    held = kv_buffer.shape[1] // head_width
    pages = (
        gathered.reshape(KEY_VALUE_HEADS // held, blocks, PAGE_TOKENS, held, head_width)
        .transpose(0, 3, 1, 2, 4)
        .reshape(KEY_VALUE_HEADS * blocks, PAGE_TOKENS * head_width)
    )
    slots = tp_rank * cache_page_count + jnp.arange(cache_page_count, dtype=jnp.int32)
    onehot = (page_rows.reshape(-1)[None, :] == slots[:, None]).astype(jnp.bfloat16)
    picked = jnp.dot(onehot, pages, preferred_element_type=jnp.float32).astype(jnp.bfloat16)
    return picked.reshape(cache_page_count, PAGE_TOKENS, head_width)


def body(tokens, gain, q_weight, kv_weight, out_weight, page_table, segment_ids):
    tensor_parallel_width = lax.axis_size("tp")
    pp_size = lax.axis_size("pp")
    tp_rank = lax.axis_index("tp")
    section_idx = lax.axis_index("pp")
    w_query = q_weight[0]
    w_keyval = kv_weight[0]
    w_output = out_weight[0]
    page_rows = page_table[0]
    local_width = tokens.shape[1]
    row_total = tokens.shape[0]
    row_count = row_total // MICRO_BATCHES
    head_dim = HEAD_SIZE
    kv_cols = w_keyval.shape[1]
    held_heads = max(1, kv_cols // (2 * head_dim))
    q_heads = w_query.shape[1] // head_dim
    per_kv = q_heads // held_heads
    cache_page_count = KEY_VALUE_HEADS * (row_total // PAGE_TOKENS) // tensor_parallel_width
    score_scale = 1.0 / math.sqrt(head_dim)
    step_count = MICRO_BATCHES + pp_size - 1
    key_pos = jnp.arange(row_total, dtype=jnp.int32)

    def add_columns(block_cols):
        return (
            jnp.dot(block_cols, w_query, preferred_element_type=jnp.float32),
            jnp.dot(block_cols, w_keyval, preferred_element_type=jnp.float32),
        )

    def add_outputs(block_cols):
        return jnp.dot(block_cols, w_output, preferred_element_type=jnp.float32)

    def one_step(step_idx, state_tuple):
        received, kv_buffer, collected = state_tuple
        micro_raw = step_idx - section_idx
        is_live = (micro_raw >= 0) & (micro_raw < MICRO_BATCHES)
        micro_idx = jnp.clip(micro_raw, 0, MICRO_BATCHES - 1)
        row_start = micro_idx * row_count
        first_rows = lax.dynamic_slice_in_dim(tokens, row_start, row_count, 0)
        current = jnp.where(section_idx == 0, first_rows, received)
        widened = current.astype(jnp.float32)
        partial_sq = jnp.sum(widened * widened, axis=1, keepdims=True)
        mean_sq = lax.psum(partial_sq, "tp") / MODEL_WIDTH
        normed = (widened * lax.rsqrt(mean_sq + eps_norm) * gain.astype(jnp.float32)).astype(
            jnp.bfloat16
        )
        query_sum, keyval_sum = add_columns(lax.all_gather(normed, "tp", axis=1, tiled=True))
        query_matrix = query_sum.astype(jnp.bfloat16)
        kv_own = keyval_sum.astype(jnp.bfloat16)
        if tensor_parallel_width > KEY_VALUE_HEADS:
            partner = partner_2(kv_own, "tp", 0)
            first_half = tp_rank % 2 == 0
            head_pair = jnp.where(
                first_half,
                jnp.concatenate([kv_own, partner], axis=1),
                jnp.concatenate([partner, kv_own], axis=1),
            )
        else:
            head_pair = kv_own
        refreshed = lax.dynamic_update_slice_in_dim(kv_buffer, head_pair, row_start, 0)
        kv_buffer = jnp.where(is_live, refreshed, kv_buffer)
        kv_view = kv_buffer.reshape(row_total, held_heads, 2, head_dim)
        grouped_queries = query_matrix.reshape(row_count, held_heads, per_kv, head_dim)
        scores = (
            jnp.einsum(
                "qgpd,kgd->gpqk",
                grouped_queries,
                kv_view[:, :, 0],
                preferred_element_type=jnp.float32,
            )
            * score_scale
        )
        query_pos = row_start + jnp.arange(row_count, dtype=jnp.int32)
        seg_query = lax.dynamic_slice_in_dim(segment_ids, row_start, row_count, 0)
        allowed = (key_pos[None, :] <= query_pos[:, None]) & (
            segment_ids[None, :] == seg_query[:, None]
        )
        scores = jnp.where(allowed[None, None], scores, -1e30)
        row_max = jnp.max(scores, axis=-1, keepdims=True)
        raised = jnp.exp(scores - row_max)
        weights = (raised / jnp.sum(raised, axis=-1, keepdims=True)).astype(jnp.bfloat16)
        attended = jnp.einsum(
            "gpqk,kgd->qgpd", weights, kv_view[:, :, 1], preferred_element_type=jnp.float32
        )
        attended = attended.astype(jnp.bfloat16).reshape(row_count, q_heads * head_dim)
        projected = add_outputs(lax.all_gather(attended, "tp", axis=1, tiled=True))
        produced = (widened + projected).astype(jnp.bfloat16)
        placed = lax.dynamic_update_slice_in_dim(collected, produced, row_start, 0)
        collected = jnp.where(is_live & (section_idx == pp_size - 1), placed, collected)
        handed = shifted(produced, "pp", 1)
        return (handed, kv_buffer, collected)

    initial = (
        jnp.zeros((row_count, local_width), jnp.bfloat16),
        jnp.zeros((row_total, held_heads * 2 * head_dim), jnp.bfloat16),
        jnp.zeros((row_total, local_width), jnp.bfloat16),
    )
    finished = lax.fori_loop(0, step_count, one_step, initial)
    whole_final = from_root(finished[2], "pp", pp_size - 1)
    share_rows = row_total // pp_size
    hidden = lax.dynamic_slice_in_dim(whole_final, section_idx * share_rows, share_rows, 0)
    kv_cache = own_pages(
        finished[1], page_rows, tp_rank, tensor_parallel_width, cache_page_count
    )
    return (hidden, kv_cache[None])


def solution(mesh):
    placed = (
        P("grp", "tp"),
        P("pp", "tp"),
        P("pp", None, "tp"),
        P("pp", None, "tp"),
        P("pp", None, "tp"),
        P("pp", None, None),
        P("grp"),
    )
    return jax.shard_map(
        body,
        mesh=mesh,
        in_specs=placed,
        out_specs=(P(("grp", "pp"), "tp"), P("pp", ("grp", "tp"), None, None)),
        check_vma=False,
    )
```

```python
import math

import jax
import jax.numpy as jnp
from jax import lax
from jax.sharding import PartitionSpec as P

MODEL_WIDTH = 8192
HEAD_SIZE = 128
KEY_VALUE_HEADS = 8
PAGE_TOKENS = 4


eps_norm = 1e-05


def partner_2(x, axis, apart):
    return lax.ppermute(x, axis, [(i, i ^ 1 << apart) for i in range(lax.axis_size(axis))])


def shifted(x, axis, by):
    peers = lax.axis_size(axis)
    pairs = [(i, i + by) for i in range(peers) if 0 <= i + by < peers]
    return lax.ppermute(x, axis, pairs)


def own_pages(kv_buffer, page_rows, tp_rank, tensor_parallel_width, cache_page_count):
    row_total = kv_buffer.shape[0]
    blocks = row_total // PAGE_TOKENS
    copies = max(1, tensor_parallel_width // KEY_VALUE_HEADS)
    gathered = lax.all_gather(kv_buffer, "tp", axis=0, tiled=False)[::copies]
    head_width = 2 * HEAD_SIZE
    held = kv_buffer.shape[1] // head_width
    pages = (
        gathered.reshape(KEY_VALUE_HEADS // held, blocks, PAGE_TOKENS, held, head_width)
        .transpose(0, 3, 1, 2, 4)
        .reshape(KEY_VALUE_HEADS * blocks, PAGE_TOKENS * head_width)
    )
    slots = tp_rank * cache_page_count + jnp.arange(cache_page_count, dtype=jnp.int32)
    onehot = (page_rows.reshape(-1)[None, :] == slots[:, None]).astype(jnp.bfloat16)
    picked = jnp.dot(onehot, pages, preferred_element_type=jnp.float32).astype(jnp.bfloat16)
    return picked.reshape(cache_page_count, PAGE_TOKENS, head_width)


def body(tokens, gain, q_weight, kv_weight, out_weight, page_table, segment_ids):
    tensor_parallel_width = lax.axis_size("tp")
    pp_size = lax.axis_size("pp")
    tp_rank = lax.axis_index("tp")
    section_idx = lax.axis_index("pp")
    w_query = q_weight[0]
    w_keyval = kv_weight[0]
    w_output = out_weight[0]
    page_rows = page_table[0]
    local_width = tokens.shape[1]
    row_total = tokens.shape[0]
    micro_batches = pp_size
    row_count = row_total // micro_batches
    head_dim = HEAD_SIZE
    kv_cols = w_keyval.shape[1]
    held_heads = max(1, kv_cols // (2 * head_dim))
    q_heads = w_query.shape[1] // head_dim
    per_kv = q_heads // held_heads
    cache_page_count = KEY_VALUE_HEADS * (row_total // PAGE_TOKENS) // tensor_parallel_width
    score_scale = 1.0 / math.sqrt(head_dim)
    step_count = micro_batches + pp_size - 1
    gain_all = lax.all_gather(gain, "tp", axis=1, tiled=True).astype(jnp.float32)

    def add_columns(block_cols):
        return (
            jnp.dot(block_cols, w_query, preferred_element_type=jnp.float32),
            jnp.dot(block_cols, w_keyval, preferred_element_type=jnp.float32),
        )

    def add_outputs(block_cols):
        return jnp.dot(block_cols, w_output, preferred_element_type=jnp.float32)

    def one_step(step_idx, state_tuple):
        received, kv_buffer, hidden = state_tuple
        micro_raw = step_idx - section_idx
        is_live = (micro_raw >= 0) & (micro_raw < micro_batches)
        micro_idx = jnp.clip(micro_raw, 0, micro_batches - 1)
        row_start = micro_idx * row_count
        first_rows = lax.dynamic_slice_in_dim(tokens, row_start, row_count, 0)
        current = jnp.where(section_idx == 0, first_rows, received)
        whole_rows = lax.all_gather(current, "tp", axis=1, tiled=True).astype(jnp.float32)
        mean_sq = jnp.sum(whole_rows * whole_rows, axis=1, keepdims=True) / MODEL_WIDTH
        normed = (whole_rows * lax.rsqrt(mean_sq + eps_norm) * gain_all).astype(jnp.bfloat16)
        query_sum, keyval_sum = add_columns(normed)
        query_matrix = query_sum.astype(jnp.bfloat16)
        kv_own = keyval_sum.astype(jnp.bfloat16)
        if tensor_parallel_width > KEY_VALUE_HEADS:
            partner = partner_2(kv_own, "tp", 0)
            first_half = tp_rank % 2 == 0
            head_pair = jnp.where(
                first_half,
                jnp.concatenate([kv_own, partner], axis=1),
                jnp.concatenate([partner, kv_own], axis=1),
            )
        else:
            head_pair = kv_own
        refreshed = lax.dynamic_update_slice_in_dim(kv_buffer, head_pair, row_start, 0)
        kv_buffer = jnp.where(is_live, refreshed, kv_buffer)
        key_count = row_count * min(step_idx + 1, micro_batches)
        key_pos = jnp.arange(key_count, dtype=jnp.int32)
        kv_view = kv_buffer[:key_count].reshape(key_count, held_heads, 2, head_dim)
        grouped_queries = query_matrix.reshape(row_count, held_heads, per_kv, head_dim)
        scores = (
            jnp.einsum(
                "qgpd,kgd->gpqk",
                grouped_queries,
                kv_view[:, :, 0],
                preferred_element_type=jnp.float32,
            )
            * score_scale
        )
        query_pos = row_start + jnp.arange(row_count, dtype=jnp.int32)
        seg_query = lax.dynamic_slice_in_dim(segment_ids, row_start, row_count, 0)
        allowed = (key_pos[None, :] <= query_pos[:, None]) & (
            segment_ids[None, :key_count] == seg_query[:, None]
        )
        scores = jnp.where(allowed[None, None], scores, -1e30)
        row_max = jnp.max(scores, axis=-1, keepdims=True)
        raised = jnp.exp(scores - row_max)
        weights = (raised / jnp.sum(raised, axis=-1, keepdims=True)).astype(jnp.bfloat16)
        attended = jnp.einsum(
            "gpqk,kgd->qgpd", weights, kv_view[:, :, 1], preferred_element_type=jnp.float32
        )
        attended = attended.astype(jnp.bfloat16).reshape(row_count, q_heads * head_dim)
        projected = add_outputs(lax.all_gather(attended, "tp", axis=1, tiled=True))
        produced = (current.astype(jnp.float32) + projected).astype(jnp.bfloat16)
        done = step_idx - (pp_size - 1)
        if done >= 0:
            share = produced
            if done < pp_size - 1:
                share = lax.ppermute(produced, "pp", [(pp_size - 1, done)])
            hidden = jnp.where(section_idx == done, share, hidden)
        handed = shifted(produced, "pp", 1) if step_idx < step_count - 1 else produced
        return (handed, kv_buffer, hidden)

    initial = (
        jnp.zeros((row_count, local_width), jnp.bfloat16),
        jnp.zeros((row_total, held_heads * 2 * head_dim), jnp.bfloat16),
        jnp.zeros((row_count, local_width), jnp.bfloat16),
    )
    finished = initial
    for step_idx in range(step_count):
        finished = one_step(step_idx, finished)
    hidden = finished[2]
    kv_cache = own_pages(
        finished[1], page_rows, tp_rank, tensor_parallel_width, cache_page_count
    )
    return (hidden, kv_cache[None])


def solution(mesh):
    placed = (
        P("grp", "tp"),
        P("pp", "tp"),
        P("pp", None, "tp"),
        P("pp", None, "tp"),
        P("pp", None, "tp"),
        P("pp", None, None),
        P("grp"),
    )
    return jax.shard_map(
        body,
        mesh=mesh,
        in_specs=placed,
        out_specs=(P(("grp", "pp"), "tp"), P("pp", ("grp", "tp"), None, None)),
        check_vma=False,
    )
```
